512 devices in a mesh: tm: 2 (over y_lo), space: 64 (over y_hi, z, core), member: 4 (over x).
Axes of the slice: x: 4, y: 8 (y_hi: 4, y_lo: 2; y = y_hi * 2 + y_lo), z: 8, core: 2. Of those that a mesh axis runs over, the one named last changes fastest.
Arguments:
- obs_anom: bfloat16 [6, 2, 128, 256, 1024], P('tm', None, 'space', 'member'), may hold values from -0.59375 to 0.59375
- obs_prec: bfloat16 [6, 2, 128, 1024], P('tm', None, 'space'), may hold values from 0.29882812 to 3
- innov: bfloat16 [6, 2, 128, 1024], P('tm', None, 'space'), may hold values from -6 to 6
- obs_column: int32 [6, 2, 128, 1024], P('tm', None, 'space'), may hold values from 0 to 127
- cutoff: int32 [2, 128], replicated, may hold values from 1 to 2
- inv_root: float32 [2, 128, 256, 256], P('tm', 'space'), may hold values from -0.12 to 0.12
- state_anom: bfloat16 [2, 128, 256, 32, 128], P('tm', 'space', None, 'member'), may hold values from -6 to 6
- state_mean: float32 [2, 128, 32, 128], P('tm', 'space', 'member'), may hold values from -6 to 6
Outputs:
- analysis: bfloat16 [2, 128, 256, 32, 128], P('tm', 'space', None, 'member')
The draws below stay inside these ranges and needn't reach their ends.
All inputs are finite; a program needn't handle non-finite values.
Results may differ from the reference program's by a relative error of at most 0.0062.
Values may be sent and summed in bfloat16 or wider, within the bound.
A program may use at most 64 MiB of HBM per device.

```python
import math
import jax
import jax.numpy as jnp
from jax import lax

K = 256
SLOTS = 6
OBS = 1024
HALO = 2
LEVELS = 32
POINTS = 128
NEWTON = 2
SECTORS = 2
TILES_SEC = 128


def common_factor(key):
    return jax.random.uniform(jax.random.fold_in(key, 11), (K,), jnp.float32, -2.0, 2.0)


def draw_obs_anom(key, part):
    extent = (SLOTS, SECTORS, TILES_SEC, K, OBS)
    code_extent = (SLOTS, SECTORS, TILES_SEC, 1, OBS)
    spread = 3.8 / math.sqrt(OBS)
    factor = common_factor(key)
    noise_key = jax.random.fold_in(key, 3)
    code_key = jax.random.fold_in(key, 5)
    share = 0.3
    noise_draw = jax.random.truncated_normal(noise_key, -3.0, 3.0, extent, jnp.float32)
    codes = jax.random.truncated_normal(code_key, -2.0, 2.0, code_extent, jnp.float32)
    values = math.sqrt(1.0 - share) * noise_draw + math.sqrt(share) * factor[:, None] * codes
    return (values * spread).astype(jnp.bfloat16)


def draw_inv_root(key, part):
    extent = (SECTORS, TILES_SEC, K, K)
    spread = 0.1 / math.sqrt(K)
    total = 108.0 * (HALO / 2 + 1)
    factor = common_factor(key)
    direction = factor / jnp.sqrt(jnp.sum(factor * factor))
    noise_key = jax.random.fold_in(key, 7)
    share = 0.3
    noise_draw = jax.random.truncated_normal(noise_key, -4.0, 4.0, extent, jnp.float32)
    centre = 1.0 / math.sqrt(K - 1 + total * (1.0 - share))
    along = 1.0 / jnp.sqrt(K - 1 + total * (1.0 - share + share * jnp.sum(factor * factor)))
    symmetric = (noise_draw + jnp.swapaxes(noise_draw, -1, -2)) * (spread / math.sqrt(2.0))
    identity = jnp.eye(K, dtype=jnp.float32)
    outer_dir = direction[:, None] * direction[None, :]
    project = identity - outer_dir
    symmetric = jnp.einsum('ij,stjk,kl->stil', project, symmetric, project, precision=jax.lax.Precision.HIGHEST)
    result = centre * (identity + symmetric) + (along - centre) * outer_dir
    return result.astype(jnp.float32)


def touch_ends(values, stream_key, low, high):
    longest = values.shape.index(max(values.shape))
    spots = []
    for shift in (0, 1):
        where = [jax.random.randint(jax.random.fold_in(stream_key, axis), (), 0, length) for axis, length in enumerate(values.shape)]
        where[longest] = (where[longest] + shift) % values.shape[longest]
        spots.append(tuple(where))
    return values.at[spots[0]].set(low).at[spots[1]].set(high)


def shard_levels(own_key, shape, cuts, least, top_value):
    def one(axis_at, blocks):
        draws = jax.random.uniform(jax.random.fold_in(jax.random.fold_in(own_key, 6), axis_at), (blocks,), jnp.float32, least / len(cuts), top_value / len(cuts))
        return jnp.repeat(jnp.exp(draws), shape[axis_at] // blocks).reshape((-1,) + (1,) * (len(shape) - axis_at - 1))

    level = one(*cuts[0])
    for cut in cuts[1:]:
        level = level * one(*cut)
    return level


def scatter_about(own_key, shape, deviation, bound, shards=(), kind=jnp.bfloat16):
    values = jax.random.normal(own_key, shape, jnp.float32) * deviation
    if len(shards) > 0:
        values = shard_levels(own_key, shape, shards, -0.22, 0.18) * values
    return jnp.clip(values, min=-bound, max=bound).astype(kind)


def setup_inputs(seed: int = 0) -> dict:
    key_list = jax.random.split(jax.random.key(seed), 9)
    return {
        "obs_anom": draw_obs_anom(jax.random.fold_in(key_list[8], 71), 0),
        "obs_prec": jnp.clip(jnp.exp(math.log(3.0) - 2.306499 * jax.random.uniform(key_list[1], (SLOTS, SECTORS, TILES_SEC, OBS), jnp.float32) ** shard_levels(key_list[1], (SLOTS, SECTORS, TILES_SEC, OBS), ((0, 2), (2, 64)), -0.2, 0.2)), 0.29882812, 3.0).astype(jnp.bfloat16),
        "innov": scatter_about(key_list[2], (SLOTS, SECTORS, TILES_SEC, OBS), 1.0, 6.0, ((0, 2), (2, 64))),
        "obs_column": touch_ends(jax.random.randint(key_list[3], (SLOTS, SECTORS, TILES_SEC, OBS), 0, POINTS), jax.random.fold_in(key_list[3], 1), 0, POINTS - 1).astype(jnp.int32),
        "cutoff": touch_ends(jax.random.randint(key_list[4], (SECTORS, TILES_SEC), 1, HALO + 1), jax.random.fold_in(key_list[4], 1), 1, HALO).astype(jnp.int32),
        "inv_root": draw_inv_root(jax.random.fold_in(key_list[8], 71), 0),
        "state_anom": scatter_about(key_list[6], (SECTORS, TILES_SEC, K, LEVELS, POINTS), 1.0, 6.0, ((0, 2), (1, 64), (3, 4))),
        "state_mean": scatter_about(key_list[7], (SECTORS, TILES_SEC, LEVELS, POINTS), 1.0, 6.0, ((0, 2), (1, 64), (2, 4)), jnp.float32),
    }


def taper_weight(distance, reach_now, columns):
    scaled_reach = (reach_now + 0.5) * columns
    relative = distance / scaled_reach
    return jnp.square(jnp.maximum(1.0 - relative * relative, 0.0))

def reference(obs_anom, obs_prec, innov, obs_column, cutoff, inv_root, state_anom, state_mean):
    tile_total = SECTORS * TILES_SEC
    anomaly = obs_anom.reshape(SLOTS, tile_total, K, OBS)
    precision = obs_prec.reshape(SLOTS, tile_total, OBS).astype(jnp.float32)
    innovation = innov.reshape(SLOTS, tile_total, OBS).astype(jnp.float32)
    placing = obs_column.reshape(SLOTS, tile_total, OBS).astype(jnp.float32) + (0.5 - POINTS / 2)
    reaches = cutoff.reshape(tile_total).astype(jnp.float32)
    root_all = inv_root.reshape(tile_total, K, K)
    anomalies = state_anom.reshape(tile_total, K, LEVELS * POINTS)
    mean_rows = state_mean.reshape(tile_total, 1, LEVELS * POINTS)
    offsets = jnp.arange(-HALO, HALO + 1, dtype=jnp.int32)
    shifts = offsets.astype(jnp.float32)
    identity = jnp.eye(K, dtype=jnp.float32)
    highest = lax.Precision.HIGHEST

    def analyse(tile_index):
        beside_all = (tile_index + offsets + tile_total) % tile_total
        window = jnp.take(anomaly, beside_all, axis=1)
        window_prec = jnp.take(precision, beside_all, axis=1)
        window_innov = jnp.take(innovation, beside_all, axis=1)
        window_place = jnp.take(placing, beside_all, axis=1)
        distance = shifts[None, :, None] * POINTS + window_place
        coeffs = taper_weight(distance, reaches[tile_index], POINTS) * window_prec
        scaled = (window.astype(jnp.float32) * coeffs[:, :, None, :]).astype(jnp.bfloat16)
        weighted = (coeffs * window_innov).astype(jnp.bfloat16)
        gram_part = jnp.einsum('swko,swlo->kl', scaled.astype(jnp.float32), window.astype(jnp.float32))
        proj_part = jnp.einsum('swko,swo->k', window.astype(jnp.float32), weighted.astype(jnp.float32))
        system = (K - 1.0) * identity + gram_part
        inv_sqrt = root_all[tile_index]
        for newton_step in range(NEWTON):
            square = jnp.dot(inv_sqrt, inv_sqrt, precision=highest)
            applied = jnp.dot(system, square, precision=highest)
            inv_sqrt = 1.5 * inv_sqrt - 0.5 * jnp.dot(inv_sqrt, applied, precision=highest)
        mean_weight = jnp.dot(inv_sqrt, jnp.dot(inv_sqrt, proj_part, precision=highest), precision=highest)
        weights = (mean_weight[:, None] + math.sqrt(K - 1) * inv_sqrt).astype(jnp.bfloat16)
        result = mean_rows[tile_index] + jnp.dot(weights.T, anomalies[tile_index], preferred_element_type=jnp.float32)
        return result.astype(jnp.bfloat16)
    analysis = lax.map(analyse, jnp.arange(tile_total, dtype=jnp.int32))
    return analysis.reshape(SECTORS, TILES_SEC, K, LEVELS, POINTS)
```

```python
import functools
import math

import jax
import jax.numpy as jnp
from jax import lax
from jax.experimental import pallas as pl
from jax.experimental.pallas import tpu as pltpu
from jax.sharding import PartitionSpec as P

MESH = pl.DeviceIdType.MESH
K = 256
POINTS = 128
NEWTON = 2
CHUNKS = 6
WIDTH = 512
WIN = 5
NEAR = 192
LATE = WIN * 64 + 16
F32 = jnp.float32
BF16 = jnp.bfloat16


def nt_dot(a, b):
    return lax.dot_general(a, b, (((1,), (1,)), ((), ())), preferred_element_type=F32)


def split(a):
    hi = a.astype(BF16)
    return hi, (a - hi.astype(F32)).astype(BF16)


def mm(a, b):
    return jnp.dot(a, b, preferred_element_type=F32)


def mm3(a, b):
    (ah, al), (bh, bl) = a, b
    return mm(ah, bh) + (mm(ah, bl) + mm(al, bh))


def gather_kernel(
    obs_ref, prec_ref, innov_ref, col_ref, cut_hbm, state_ref, root_hbm,
    gram_out, proj_out, flat_out, square_out,
    data, prec_v, innov_v, col_v, cut_ref, coef, wgt, lhs_e, lhs_f, acc_e, acc_f,
    send_e, got_e, send_f, got_f, send_p, got_p, all_e, all_f, all_p, strip, state_v, root_v, tmp,
    info_sem, state_sem, info_send, info_recv, a2a_send, a2a_recv,
    e_send, e_recv, f_send, f_recv, p_send, p_recv, eb_send, eb_recv, fb_send, fb_recv, pb_send, pb_recv,
):
    tm = lax.axis_index("tm")
    s = lax.axis_index("space")
    x = lax.axis_index("member")
    ns = 64
    i = lax.rem(x, 2)
    half = x // 2
    pair = tm * ns + s
    other = 1 - tm

    def pair_at(p):
        q = lax.rem(p + 2 * ns, 2 * ns)
        return {"tm": q // ns, "space": lax.rem(q, ns)}

    lower, upper = pair_at(pair - 1), pair_at(pair + 1)

    def peer(h, k):
        return {"tm": lax.rem(tm + h, 2), "member": lax.rem(x + k, 4)}

    place = {1: 0, 0: 1, 3: 2, 2: 3}

    own = [
        pltpu.make_async_copy(
            obs_ref.at[c, tm, i, :, pl.ds(pl.multiple_of(half * WIDTH, WIDTH), WIDTH)],
            data.at[c, 64:128, :],
            a2a_recv.at[0, 0, c],
        )
        for c in range(3)
    ]
    for cp in own:
        cp.start()
    infos = [(prec_ref, prec_v), (innov_ref, innov_v), (col_ref, col_v)]
    local = [pltpu.make_async_copy(a.at[:, tm], b.at[0], info_sem.at[n]) for n, (a, b) in enumerate(infos)]
    for cp in local:
        cp.start()
    cut_cp = pltpu.make_async_copy(cut_hbm, cut_ref, info_sem.at[3])
    cut_cp.start()
    state_cp = pltpu.make_async_copy(state_ref.at[0], state_v, state_sem)
    state_cp.start()
    root_cp = pltpu.make_async_copy(root_hbm.at[0], root_v, info_sem.at[4])
    root_cp.start()

    barrier = pltpu.get_barrier_semaphore()
    for h in range(2):
        for k in range(4):
            if h or k:
                pl.semaphore_signal(barrier, inc=1, device_id=peer(h, k), device_id_type=MESH)
    pl.semaphore_signal(barrier, inc=1, device_id=lower, device_id_type=MESH)
    pl.semaphore_signal(barrier, inc=1, device_id=upper, device_id_type=MESH)
    pl.semaphore_wait(barrier, 9)

    def remote(src, dst, send, recv, dev):
        return pltpu.make_async_remote_copy(
            src_ref=src, dst_ref=dst, send_sem=send, recv_sem=recv, device_id=dev, device_id_type=MESH
        )

    def await_into(dst, recv):
        remote(dst, dst, info_send.at[0], recv, lower).wait_recv()

    info_cps = [
        remote(a.at[:, other], b.at[1], info_send.at[n], info_recv.at[n], {"tm": other})
        for n, (a, b) in enumerate(infos)
    ]
    for cp in info_cps:
        cp.start()

    def a2a(h, k, c):
        xp = lax.rem(x + k, 4)
        return remote(
            obs_ref.at[
                c, lax.rem(tm + h, 2), lax.rem(xp, 2), :, pl.ds(pl.multiple_of((xp // 2) * WIDTH, WIDTH), WIDTH)
            ],
            data.at[3 * h + c, pl.ds(place[k] * 64, 64), :],
            a2a_send.at[h, k, c],
            a2a_recv.at[h, k, c],
            peer(h, k),
        )

    order = [(h, k, c) for c in range(3) for h, k in ((0, 1), (0, 3), (1, 0), (1, 1), (1, 3))]
    order += [(h, 2, c) for c in range(3) for h in range(2)]
    for args in order:
        a2a(*args).start()

    z6 = jnp.where(i == 0, 5, 0)
    send_e[z6] = jnp.zeros((NEAR, 128), BF16)
    send_f[z6] = jnp.zeros((64, 256), BF16)
    send_p[z6] = jnp.zeros((1, 256), F32)

    state_cp.wait()
    for t in range(2):

        def relay(n, carry, t=t):
            block = state_v[t, pl.ds(pl.multiple_of(n * 16, 16), 16)].astype(F32)
            tmp[...] = block.reshape(128, 128)
            for level in range(8):
                flat_out[t, pl.ds(pl.multiple_of(n * 16, 16), 16), level * 128 : (level + 1) * 128] = tmp[
                    pl.ds(level, 16, stride=8), :
                ].astype(BF16)
            return carry

        lax.fori_loop(0, 16, relay, 0)

    for cp in local + [cut_cp]:
        cp.wait()
    for n, (a, b) in enumerate(infos):
        await_into(b.at[1], info_recv.at[n])
    lanes = pl.ds(pl.multiple_of(half * WIDTH, WIDTH), WIDTH)
    for c in range(CHUNKS):

        def row(ref):
            both = ref[c // 3, c % 3, :, lanes].astype(F32)
            return jnp.where(i == 0, both[0:1], both[1:2])

        prec, innov, col = row(prec_v), row(innov_v), row(col_v)
        rows, wrows = [], []
        for w in range(WIN):
            target = lax.rem(2 * pair + i + w - 2 + 4 * ns, 4 * ns)
            reach = (cut_ref[target // (2 * ns), lax.rem(target, 2 * ns)].astype(F32) + 0.5) * POINTS
            relative = (col + ((2 - w) * POINTS + 0.5 - POINTS / 2)) / reach
            taper = jnp.maximum(1.0 - relative * relative, 0.0)
            cf = taper * taper * prec
            rows.append(cf)
            wrows.append(cf * innov)
        zero = jnp.zeros((1, WIDTH), F32)
        coef[c] = jnp.concatenate(rows + [zero] * 3, axis=0)
        wgt[c] = jnp.concatenate(wrows + [zero] * 11, axis=0).astype(BF16)

    root_cp.wait()
    for t in range(2):
        part = split(root_v[t])
        square_out[t] = mm3(part, part)

    acc_e[...] = jnp.zeros_like(acc_e)
    acc_f[...] = jnp.zeros_like(acc_f)

    def near(c, carry):
        h, sl = c // 3, lax.rem(c, 3)
        for k in (0, 1, 3):
            await_into(data.at[c, place[k] * 64 : place[k] * 64 + 64, :], a2a_recv.at[h, k, sl])
        for rb in range(6):
            rows = data[c, rb * 32 : (rb + 1) * 32, :].astype(F32)
            for w in range(WIN):
                lhs_e[w * NEAR + rb * 32 : w * NEAR + (rb + 1) * 32, :] = (rows * coef[c, w : w + 1, :]).astype(BF16)
        acc_e[:, 0:NEAR] += nt_dot(lhs_e[...], data[c, 0:NEAR, :])
        return carry

    lax.fori_loop(0, CHUNKS, near, 0)
    left = lax.broadcasted_iota(jnp.int32, (64, 128), 1) < 64
    for w in range(WIN):
        w6, b = i + w, w * NEAR
        send_e[w6, 0:64, :] = jnp.where(left, acc_e[b : b + 64, 0:128], acc_e[b + 64 : b + 128, 0:128]).astype(BF16)
        send_e[w6, 64:128, :] = jnp.where(
            left, acc_e[b + 64 : b + 128, 0:128], pltpu.roll(acc_e[b + 128 : b + 192, 128:256], 64, 1)
        ).astype(BF16)
        send_e[w6, 128:192, :] = acc_e[b + 128 : b + 192, 0:128].astype(BF16)

    e_cps = [
        remote(send_e.at[0:2], got_e.at[0], e_send.at[0], e_recv.at[0], lower),
        remote(send_e.at[4:6], got_e.at[1], e_send.at[1], e_recv.at[1], upper),
    ]
    for cp in e_cps:
        cp.start()
    def late(c, carry):
        h, sl = c // 3, lax.rem(c, 3)
        await_into(data.at[c, 192:256, :], a2a_recv.at[h, 2, sl])
        for rb in range(2):
            rows = data[c, NEAR + rb * 32 : NEAR + (rb + 1) * 32, :].astype(F32)
            for w in range(WIN):
                lhs_f[w * 64 + rb * 32 : w * 64 + (rb + 1) * 32, :] = (rows * coef[c, w : w + 1, :]).astype(BF16)
        lhs_f[WIN * 64 :, :] = wgt[c]
        acc_f[...] += nt_dot(lhs_f[...], data[c])
        return carry

    lax.fori_loop(0, CHUNKS, late, 0)
    for w in range(WIN):
        w6 = i + w
        send_f[w6] = acc_f[w * 64 : w * 64 + 64, :].astype(BF16)
        send_p[w6] = acc_f[WIN * 64 + w : WIN * 64 + w + 1, :]
    f_cps = [
        remote(send_f.at[0:2], got_f.at[0], f_send.at[0], f_recv.at[0], lower),
        remote(send_f.at[4:6], got_f.at[1], f_send.at[1], f_recv.at[1], upper),
        remote(send_p.at[0:2], got_p.at[0], p_send.at[0], p_recv.at[0], lower),
        remote(send_p.at[4:6], got_p.at[1], p_send.at[1], p_recv.at[1], upper),
    ]
    for cp in f_cps:
        cp.start()
    for n in range(2):
        await_into(got_e.at[n], e_recv.at[n])
    for j in range(2):
        all_e[x, j] = (got_e[0, j].astype(F32) + got_e[1, j].astype(F32) + send_e[2 + j].astype(F32)).astype(BF16)
    eb_cps = [
        remote(all_e.at[x], all_e.at[x], eb_send.at[k - 1], eb_recv.at[k - 1], {"member": lax.rem(x + k, 4)})
        for k in (1, 3, 2)
    ]
    for cp in eb_cps:
        cp.start()

    for n in range(2):
        await_into(got_f.at[n], f_recv.at[n])
        await_into(got_p.at[n], p_recv.at[n])
    for j in range(2):
        all_f[x, j] = (got_f[0, j].astype(F32) + got_f[1, j].astype(F32) + send_f[2 + j].astype(F32)).astype(BF16)
        all_p[x, j] = got_p[0, j] + got_p[1, j] + send_p[2 + j]
    fb_cps = []
    for k in (1, 3, 2):
        fb_cps.append(
            remote(all_f.at[x], all_f.at[x], fb_send.at[k - 1], fb_recv.at[k - 1], {"member": lax.rem(x + k, 4)})
        )
        fb_cps.append(
            remote(all_p.at[x], all_p.at[x], pb_send.at[k - 1], pb_recv.at[k - 1], {"member": lax.rem(x + k, 4)})
        )
    for cp in fb_cps:
        cp.start()

    for cp in info_cps + [a2a(*args) for args in order] + e_cps + f_cps:
        cp.wait_send()

    def turn(value, xs):
        shift = (64 * (xs - 1)) % 256
        return pltpu.roll(value, shift, 1) if shift else value

    for k in (1, 3, 2):
        await_into(all_e.at[lax.rem(x + 4 - k, 4)], eb_recv.at[k - 1])
    side = jnp.zeros((64, 128), F32)
    for j in range(2):
        for r in range(4):
            a, b, c = (r + 1) % 4, r, (r + 3) % 4
            one = jnp.where(left, all_e[a, j, 0:64, :].astype(F32), 0.0)
            two = jnp.where(left, all_e[b, j, 64:128, :].astype(F32), all_e[b, j, 0:64, :].astype(F32))
            three = jnp.where(left, pltpu.roll(all_e[c, j, 64:128, :].astype(F32), 64, 1), 0.0)
            strip[j, 64 * r : 64 * r + 64, :] = (
                turn(jnp.concatenate([one, side], axis=1), a)
                + turn(jnp.concatenate([two, side], axis=1), b)
                + turn(jnp.concatenate([all_e[c, j, 128:192, :].astype(F32), three], axis=1), c)
            )
    off = lax.broadcasted_iota(jnp.int32, (256, 256), 0) // 64 != lax.broadcasted_iota(jnp.int32, (256, 256), 1) // 64
    for k in (1, 3, 2):
        src = lax.rem(x + 4 - k, 4)
        await_into(all_f.at[src], fb_recv.at[k - 1])
        await_into(all_p.at[src], pb_recv.at[k - 1])
    for j in range(2):
        proj = jnp.zeros((8, 256), F32)
        for r in range(4):
            far = (r + 2) % 4
            strip[j, 64 * r : 64 * r + 64, :] += turn(all_f[far, j].astype(F32), far)
            proj += turn(jnp.broadcast_to(all_p[r, j], (8, 256)), r)
        proj_out[j] = proj[0:1]
        whole = strip[j]
        gram_out[j] = whole + jnp.where(off, jnp.transpose(whole), 0.0)
    for cp in eb_cps + fb_cps:
        cp.wait_send()


def analysis_kernel(gram_ref, proj_ref, square_ref, root_ref, flat_ref, mean_ref, out_ref, tmp, done, out_sem):
    eye = (
        lax.broadcasted_iota(jnp.int32, (K, K), 0) == lax.broadcasted_iota(jnp.int32, (K, K), 1)
    ).astype(F32)
    grams = [split(gram_ref[t]) for t in range(2)]
    roots = [root_ref[0, t] for t in range(2)]
    for step in range(NEWTON):
        parts = [split(r) for r in roots]
        squares = [mm3(p, p) for p in parts] if step else [square_ref[t] for t in range(2)]
        sq_parts = [split(q) for q in squares]
        applied = [
            (K - 1.0) * squares[t] + mm3(grams[t], sq_parts[t]) for t in range(2)
        ]
        rest = [split(eye - a) for a in applied]
        roots = [roots[t] + 0.5 * mm3(parts[t], rest[t]) for t in range(2)]
    for t in range(2):
        root = roots[t]
        rh, rl = split(root)
        pr = jnp.broadcast_to(proj_ref[t], (8, K))
        ph, pl_ = split(pr)
        inner = (nt_dot(ph, rh) + (nt_dot(ph, rl) + nt_dot(pl_, rh)))[0:1]
        mean_weight = jnp.sum(root * inner, axis=1, keepdims=True)
        weights = (mean_weight + math.sqrt(K - 1) * root).astype(BF16)
        wt = jnp.transpose(weights)
        for two in range(4):
            res = mm(wt, flat_ref[t, :, two * 256 : (two + 1) * 256])
            for half in range(2):
                level = 2 * two + half
                tmp[t, pl.ds(level, K, stride=8), :] = (
                    res[:, half * 128 : (half + 1) * 128] + mean_ref[0, t, level : level + 1, :]
                )
        done[t] = tmp[t].reshape(K, 8, 128).astype(BF16)
        pltpu.make_async_copy(done.at[t], out_ref.at[0, t], out_sem.at[t]).start()
    for t in range(2):
        pltpu.make_async_copy(done.at[t], out_ref.at[0, t], out_sem.at[t]).wait()


def body(obs_anom, obs_prec, innov, obs_column, cutoff, inv_root, state_anom, state_mean):
    obs_anom, obs_prec, innov, obs_column, cutoff, state_anom, root_far = (
        pltpu.with_memory_space_constraint(a, pltpu.HBM)
        for a in (obs_anom, obs_prec, innov, obs_column, cutoff, state_anom, inv_root)
    )
    any_ = pl.BlockSpec(memory_space=pltpu.HBM)
    vm = pl.BlockSpec(memory_space=pltpu.VMEM)
    dma = pltpu.SemaphoreType.DMA
    gram, proj, flat, square = pl.pallas_call(
        gather_kernel,
        out_shape=(
            jax.ShapeDtypeStruct((2, K, K), F32),
            jax.ShapeDtypeStruct((2, 1, K), F32),
            jax.ShapeDtypeStruct((2, K, 1024), BF16),
            jax.ShapeDtypeStruct((2, K, K), F32),
        ),
        in_specs=[any_] * 7,
        out_specs=(vm,) * 4,
        scratch_shapes=[
            pltpu.VMEM((CHUNKS, K, WIDTH), BF16),
            pltpu.VMEM((2, 3, 2, 1024), BF16),
            pltpu.VMEM((2, 3, 2, 1024), BF16),
            pltpu.VMEM((2, 3, 2, 1024), jnp.int32),
            pltpu.SMEM((2, 128), jnp.int32),
            pltpu.VMEM((CHUNKS, 8, WIDTH), F32),
            pltpu.VMEM((CHUNKS, 16, WIDTH), BF16),
            pltpu.VMEM((WIN * NEAR, WIDTH), BF16),
            pltpu.VMEM((LATE, WIDTH), BF16),
            pltpu.VMEM((WIN * NEAR, 256), F32),
            pltpu.VMEM((LATE, K), F32),
            pltpu.VMEM((6, NEAR, 128), BF16),
            pltpu.VMEM((2, 2, NEAR, 128), BF16),
            pltpu.VMEM((6, 64, 256), BF16),
            pltpu.VMEM((2, 2, 64, 256), BF16),
            pltpu.VMEM((6, 1, 256), F32),
            pltpu.VMEM((2, 2, 1, 256), F32),
            pltpu.VMEM((4, 2, NEAR, 128), BF16),
            pltpu.VMEM((4, 2, 64, 256), BF16),
            pltpu.VMEM((4, 2, 1, 256), F32),
            pltpu.VMEM((2, K, K), F32),
            pltpu.VMEM((2, K, 8, 128), BF16),
            pltpu.VMEM((2, K, K), F32),
            pltpu.VMEM((128, 128), F32),
            dma((5,)),
            dma,
            dma((3,)),
            dma((3,)),
            dma((2, 4, 3)),
            dma((2, 4, 3)),
            *[dma((2,))] * 6,
            *[dma((3,))] * 6,
        ],
        compiler_params=pltpu.CompilerParams(
            collective_id=0, has_side_effects=True, vmem_limit_bytes=32 * 1024 * 1024
        ),
        name="gather",
    )(obs_anom, obs_prec, innov, obs_column, cutoff, state_anom, root_far)
    return pl.pallas_call(
        analysis_kernel,
        out_shape=jax.ShapeDtypeStruct(state_anom.shape, BF16),
        in_specs=[vm] * 6,
        out_specs=any_,
        scratch_shapes=[pltpu.VMEM((2, K * 8, 128), F32), pltpu.VMEM((2, K, 8, 128), BF16), dma((2,))],
        compiler_params=pltpu.CompilerParams(vmem_limit_bytes=32 * 1024 * 1024),
        name="analysis",
    )(gram, proj, square, inv_root, flat, state_mean)


def solution(mesh):
    in_specs = (
        P("tm", None, "space", "member", None),
        P("tm", None, "space", None),
        P("tm", None, "space", None),
        P("tm", None, "space", None),
        P(),
        P("tm", "space", None, None),
        P("tm", "space", None, "member", None),
        P("tm", "space", "member", None),
    )
    out_specs = P("tm", "space", None, "member", None)
    return jax.shard_map(body, mesh=mesh, in_specs=in_specs, out_specs=out_specs, check_vma=False)
```

```python
import functools
import math

import jax
import jax.numpy as jnp
from jax import lax
from jax.experimental import pallas as pl
from jax.experimental.pallas import tpu as pltpu
from jax.sharding import PartitionSpec as P

MESH = pl.DeviceIdType.MESH
K = 256
POINTS = 128
NEWTON = 2
CHUNKS = 6
WIDTH = 512
WIN = 5
TURN = 4
RUN = 16
NEAR = 192
LATE = WIN * 64 + 16
F32 = jnp.float32
BF16 = jnp.bfloat16


def nt_dot(a, b):
    return lax.dot_general(a, b, (((1,), (1,)), ((), ())), preferred_element_type=F32)


def split(a):
    hi = a.astype(BF16)
    return hi, (a - hi.astype(F32)).astype(BF16)


def mm(a, b):
    return jnp.dot(a, b, preferred_element_type=F32)


def mm3(a, b):
    (ah, al), (bh, bl) = a, b
    return mm(ah, bh) + (mm(ah, bl) + mm(al, bh))


def gather_kernel(
    obs_ref, prec_ref, innov_ref, col_ref, cut_hbm, state_ref, root_hbm,
    gram_out, proj_out, flat_out, square_out,
    turn_sem, data, prec_v, innov_v, col_v, cut_ref, coef, wgt, lhs_e, lhs_f, acc_e, acc_f,
    send_e, got_e, send_f, got_f, send_p, got_p, all_e, all_f, all_p, strip, state_v, root_v, tmp,
    info_sem, state_sem, info_send, info_recv, a2a_send, a2a_recv,
    e_send, e_recv, f_send, f_recv, p_send, p_recv, eb_send, eb_recv, fb_send, fb_recv, pb_send, pb_recv,
):
    tm = lax.axis_index("tm")
    s = lax.axis_index("space")
    x = lax.axis_index("member")
    ns = 64
    i = lax.rem(x, 2)
    half = x // 2
    pair = tm * ns + s
    other = 1 - tm

    def pair_at(p):
        q = lax.rem(p + 2 * ns, 2 * ns)
        return {"tm": q // ns, "space": lax.rem(q, ns)}

    lower, upper = pair_at(pair - 1), pair_at(pair + 1)

    def peer(h, k):
        return {"tm": lax.rem(tm + h, 2), "member": lax.rem(x + k, 4)}

    place = {1: 0, 0: 1, 3: 2, 2: 3}

    own = [
        pltpu.make_async_copy(
            obs_ref.at[c, tm, i, :, pl.ds(pl.multiple_of(half * WIDTH, WIDTH), WIDTH)],
            data.at[c, 64:128, :],
            a2a_recv.at[0, 0, c],
        )
        for c in range(3)
    ]
    for cp in own:
        cp.start()
    infos = [(prec_ref, prec_v), (innov_ref, innov_v), (col_ref, col_v)]
    local = [pltpu.make_async_copy(a.at[:, tm], b.at[0], info_sem.at[n]) for n, (a, b) in enumerate(infos)]
    for cp in local:
        cp.start()
    cut_cp = pltpu.make_async_copy(cut_hbm, cut_ref, info_sem.at[3])
    cut_cp.start()
    state_cp = pltpu.make_async_copy(state_ref.at[0], state_v, state_sem)
    state_cp.start()
    root_cp = pltpu.make_async_copy(root_hbm.at[0], root_v, info_sem.at[4])
    root_cp.start()

    barrier = pltpu.get_barrier_semaphore()
    for h in range(2):
        for k in range(4):
            if h or k:
                pl.semaphore_signal(barrier, inc=1, device_id=peer(h, k), device_id_type=MESH)
    pl.semaphore_signal(barrier, inc=1, device_id=lower, device_id_type=MESH)
    pl.semaphore_signal(barrier, inc=1, device_id=upper, device_id_type=MESH)
    pl.semaphore_wait(barrier, 9)

    def remote(src, dst, send, recv, dev):
        return pltpu.make_async_remote_copy(
            src_ref=src, dst_ref=dst, send_sem=send, recv_sem=recv, device_id=dev, device_id_type=MESH
        )

    def await_into(dst, recv):
        remote(dst, dst, info_send.at[0], recv, lower).wait_recv()

    info_cps = [
        remote(a.at[:, other], b.at[1], info_send.at[n], info_recv.at[n], {"tm": other})
        for n, (a, b) in enumerate(infos)
    ]
    for cp in info_cps:
        cp.start()

    def a2a(h, k, c):
        xp = lax.rem(x + k, 4)
        return remote(
            obs_ref.at[
                c, lax.rem(tm + h, 2), lax.rem(xp, 2), :, pl.ds(pl.multiple_of((xp // 2) * WIDTH, WIDTH), WIDTH)
            ],
            data.at[3 * h + c, pl.ds(place[k] * 64, 64), :],
            a2a_send.at[h, k, c],
            a2a_recv.at[h, k, c],
            peer(h, k),
        )

    order = [(h, k, c) for c in range(3) for h, k in ((0, 1), (0, 3), (1, 0), (1, 1), (1, 3))]
    order += [(h, 2, c) for c in range(3) for h in range(2)]

    def send_all():
        for args in order:
            a2a(*args).start()

    hurried = lax.rem(s, RUN) == RUN - 1
    held = lax.rem(s, RUN) == RUN - 2
    pl.when(jnp.logical_not(held))(send_all)

    z6 = jnp.where(i == 0, 5, 0)
    send_e[z6] = jnp.zeros((NEAR, 128), BF16)
    send_f[z6] = jnp.zeros((64, 256), BF16)
    send_p[z6] = jnp.zeros((1, 256), F32)

    state_cp.wait()
    for t in range(2):

        def relay(n, carry, t=t):
            block = state_v[t, pl.ds(pl.multiple_of(n * 16, 16), 16)].astype(F32)
            tmp[...] = block.reshape(128, 128)
            for level in range(8):
                flat_out[t, pl.ds(pl.multiple_of(n * 16, 16), 16), level * 128 : (level + 1) * 128] = tmp[
                    pl.ds(level, 16, stride=8), :
                ].astype(BF16)
            return carry

        lax.fori_loop(0, 16, relay, 0)

    for cp in local + [cut_cp]:
        cp.wait()
    for n, (a, b) in enumerate(infos):
        await_into(b.at[1], info_recv.at[n])
    lanes = pl.ds(pl.multiple_of(half * WIDTH, WIDTH), WIDTH)
    for c in range(CHUNKS):

        def row(ref):
            both = ref[c // 3, c % 3, :, lanes].astype(F32)
            return jnp.where(i == 0, both[0:1], both[1:2])

        prec, innov, col = row(prec_v), row(innov_v), row(col_v)
        rows, wrows = [], []
        for w in range(WIN):
            target = lax.rem(2 * pair + i + w - 2 + 4 * ns, 4 * ns)
            reach = (cut_ref[target // (2 * ns), lax.rem(target, 2 * ns)].astype(F32) + 0.5) * POINTS
            relative = (col + ((2 - w) * POINTS + 0.5 - POINTS / 2)) / reach
            taper = jnp.maximum(1.0 - relative * relative, 0.0)
            cf = taper * taper * prec
            rows.append(cf)
            wrows.append(cf * innov)
        zero = jnp.zeros((1, WIDTH), F32)
        coef[c] = jnp.concatenate(rows + [zero] * 3, axis=0)
        wgt[c] = jnp.concatenate(wrows + [zero] * 11, axis=0).astype(BF16)

    root_cp.wait()
    for t in range(2):
        part = split(root_v[t])
        square_out[t] = mm3(part, part)

    @pl.when(held)
    def _():
        pl.semaphore_wait(turn_sem, 1)
        send_all()

    acc_e[...] = jnp.zeros_like(acc_e)
    acc_f[...] = jnp.zeros_like(acc_f)

    def near(c, carry):
        h, sl = c // 3, lax.rem(c, 3)
        for k in (0, 1, 3):
            await_into(data.at[c, place[k] * 64 : place[k] * 64 + 64, :], a2a_recv.at[h, k, sl])
        for rb in range(6):
            rows = data[c, rb * 32 : (rb + 1) * 32, :].astype(F32)
            for w in range(WIN):
                lhs_e[w * NEAR + rb * 32 : w * NEAR + (rb + 1) * 32, :] = (rows * coef[c, w : w + 1, :]).astype(BF16)
        acc_e[:, 0:NEAR] += nt_dot(lhs_e[...], data[c, 0:NEAR, :])

        @pl.when(hurried & (c == TURN))
        def _():
            pl.semaphore_signal(turn_sem, inc=1, device_id={"space": s - 1}, device_id_type=MESH)

        return carry

    lax.fori_loop(0, CHUNKS, near, 0)
    left = lax.broadcasted_iota(jnp.int32, (64, 128), 1) < 64
    for w in range(WIN):
        w6, b = i + w, w * NEAR
        send_e[w6, 0:64, :] = jnp.where(left, acc_e[b : b + 64, 0:128], acc_e[b + 64 : b + 128, 0:128]).astype(BF16)
        send_e[w6, 64:128, :] = jnp.where(
            left, acc_e[b + 64 : b + 128, 0:128], pltpu.roll(acc_e[b + 128 : b + 192, 128:256], 64, 1)
        ).astype(BF16)
        send_e[w6, 128:192, :] = acc_e[b + 128 : b + 192, 0:128].astype(BF16)

    e_cps = [
        remote(send_e.at[0:2], got_e.at[0], e_send.at[0], e_recv.at[0], lower),
        remote(send_e.at[4:6], got_e.at[1], e_send.at[1], e_recv.at[1], upper),
    ]
    for cp in e_cps:
        cp.start()
    def late(c, carry):
        h, sl = c // 3, lax.rem(c, 3)
        await_into(data.at[c, 192:256, :], a2a_recv.at[h, 2, sl])
        for rb in range(2):
            rows = data[c, NEAR + rb * 32 : NEAR + (rb + 1) * 32, :].astype(F32)
            for w in range(WIN):
                lhs_f[w * 64 + rb * 32 : w * 64 + (rb + 1) * 32, :] = (rows * coef[c, w : w + 1, :]).astype(BF16)
        lhs_f[WIN * 64 :, :] = wgt[c]
        acc_f[...] += nt_dot(lhs_f[...], data[c])
        return carry

    lax.fori_loop(0, CHUNKS, late, 0)
    for w in range(WIN):
        w6 = i + w
        send_f[w6] = acc_f[w * 64 : w * 64 + 64, :].astype(BF16)
        send_p[w6] = acc_f[WIN * 64 + w : WIN * 64 + w + 1, :]
    f_cps = [
        remote(send_f.at[0:2], got_f.at[0], f_send.at[0], f_recv.at[0], lower),
        remote(send_f.at[4:6], got_f.at[1], f_send.at[1], f_recv.at[1], upper),
        remote(send_p.at[0:2], got_p.at[0], p_send.at[0], p_recv.at[0], lower),
        remote(send_p.at[4:6], got_p.at[1], p_send.at[1], p_recv.at[1], upper),
    ]
    for cp in f_cps:
        cp.start()
    for n in range(2):
        await_into(got_e.at[n], e_recv.at[n])
    for j in range(2):
        all_e[x, j] = (got_e[0, j].astype(F32) + got_e[1, j].astype(F32) + send_e[2 + j].astype(F32)).astype(BF16)
    eb_cps = [
        remote(all_e.at[x], all_e.at[x], eb_send.at[k - 1], eb_recv.at[k - 1], {"member": lax.rem(x + k, 4)})
        for k in (1, 3, 2)
    ]
    for cp in eb_cps:
        cp.start()

    for n in range(2):
        await_into(got_f.at[n], f_recv.at[n])
        await_into(got_p.at[n], p_recv.at[n])
    for j in range(2):
        all_f[x, j] = (got_f[0, j].astype(F32) + got_f[1, j].astype(F32) + send_f[2 + j].astype(F32)).astype(BF16)
        all_p[x, j] = got_p[0, j] + got_p[1, j] + send_p[2 + j]
    fb_cps = []
    for k in (1, 3, 2):
        fb_cps.append(
            remote(all_f.at[x], all_f.at[x], fb_send.at[k - 1], fb_recv.at[k - 1], {"member": lax.rem(x + k, 4)})
        )
        fb_cps.append(
            remote(all_p.at[x], all_p.at[x], pb_send.at[k - 1], pb_recv.at[k - 1], {"member": lax.rem(x + k, 4)})
        )
    for cp in fb_cps:
        cp.start()

    for cp in info_cps + [a2a(*args) for args in order] + e_cps + f_cps:
        cp.wait_send()

    def turn(value, xs):
        shift = (64 * (xs - 1)) % 256
        return pltpu.roll(value, shift, 1) if shift else value

    for k in (1, 3, 2):
        await_into(all_e.at[lax.rem(x + 4 - k, 4)], eb_recv.at[k - 1])
    side = jnp.zeros((64, 128), F32)
    for j in range(2):
        for r in range(4):
            a, b, c = (r + 1) % 4, r, (r + 3) % 4
            one = jnp.where(left, all_e[a, j, 0:64, :].astype(F32), 0.0)
            two = jnp.where(left, all_e[b, j, 64:128, :].astype(F32), all_e[b, j, 0:64, :].astype(F32))
            three = jnp.where(left, pltpu.roll(all_e[c, j, 64:128, :].astype(F32), 64, 1), 0.0)
            strip[j, 64 * r : 64 * r + 64, :] = (
                turn(jnp.concatenate([one, side], axis=1), a)
                + turn(jnp.concatenate([two, side], axis=1), b)
                + turn(jnp.concatenate([all_e[c, j, 128:192, :].astype(F32), three], axis=1), c)
            )
    off = lax.broadcasted_iota(jnp.int32, (256, 256), 0) // 64 != lax.broadcasted_iota(jnp.int32, (256, 256), 1) // 64
    for k in (1, 3, 2):
        src = lax.rem(x + 4 - k, 4)
        await_into(all_f.at[src], fb_recv.at[k - 1])
        await_into(all_p.at[src], pb_recv.at[k - 1])
    for j in range(2):
        proj = jnp.zeros((8, 256), F32)
        for r in range(4):
            far = (r + 2) % 4
            strip[j, 64 * r : 64 * r + 64, :] += turn(all_f[far, j].astype(F32), far)
            proj += turn(jnp.broadcast_to(all_p[r, j], (8, 256)), r)
        proj_out[j] = proj[0:1]
        whole = strip[j]
        gram_out[j] = whole + jnp.where(off, jnp.transpose(whole), 0.0)
    for cp in eb_cps + fb_cps:
        cp.wait_send()


def analysis_kernel(gram_ref, proj_ref, square_ref, root_ref, flat_ref, mean_ref, out_ref, tmp, done, out_sem):
    eye = (
        lax.broadcasted_iota(jnp.int32, (K, K), 0) == lax.broadcasted_iota(jnp.int32, (K, K), 1)
    ).astype(F32)
    grams = [split(gram_ref[t]) for t in range(2)]
    roots = [root_ref[0, t] for t in range(2)]
    for step in range(NEWTON):
        parts = [split(r) for r in roots]
        squares = [mm3(p, p) for p in parts] if step else [square_ref[t] for t in range(2)]
        sq_parts = [split(q) for q in squares]
        applied = [
            (K - 1.0) * squares[t] + mm3(grams[t], sq_parts[t]) for t in range(2)
        ]
        rest = [(0.5 * (eye - a)).astype(BF16) for a in applied]
        roots = [roots[t] + mm(parts[t][0], rest[t]) for t in range(2)]
    for t in range(2):
        root = roots[t]
        rh, rl = split(root)
        pr = jnp.broadcast_to(proj_ref[t], (8, K))
        ph, pl_ = split(pr)
        inner = (nt_dot(ph, rh) + (nt_dot(ph, rl) + nt_dot(pl_, rh)))[0:1]
        mean_weight = jnp.sum(root * inner, axis=1, keepdims=True)
        weights = (mean_weight + math.sqrt(K - 1) * root).astype(BF16)
        wt = jnp.transpose(weights)
        for two in range(4):
            res = mm(wt, flat_ref[t, :, two * 256 : (two + 1) * 256])
            for half in range(2):
                level = 2 * two + half
                tmp[t, pl.ds(level, K, stride=8), :] = (
                    res[:, half * 128 : (half + 1) * 128] + mean_ref[0, t, level : level + 1, :]
                )
        done[t] = tmp[t].reshape(K, 8, 128).astype(BF16)
        pltpu.make_async_copy(done.at[t], out_ref.at[0, t], out_sem.at[t]).start()
    for t in range(2):
        pltpu.make_async_copy(done.at[t], out_ref.at[0, t], out_sem.at[t]).wait()


def body(obs_anom, obs_prec, innov, obs_column, cutoff, inv_root, state_anom, state_mean):
    obs_anom, obs_prec, innov, obs_column, cutoff, state_anom, root_far = (
        pltpu.with_memory_space_constraint(a, pltpu.HBM)
        for a in (obs_anom, obs_prec, innov, obs_column, cutoff, state_anom, inv_root)
    )
    any_ = pl.BlockSpec(memory_space=pltpu.HBM)
    vm = pl.BlockSpec(memory_space=pltpu.VMEM)
    dma = pltpu.SemaphoreType.DMA
    gram, proj, flat, square = pl.pallas_call(
        gather_kernel,
        out_shape=(
            jax.ShapeDtypeStruct((2, K, K), F32),
            jax.ShapeDtypeStruct((2, 1, K), F32),
            jax.ShapeDtypeStruct((2, K, 1024), BF16),
            jax.ShapeDtypeStruct((2, K, K), F32),
        ),
        in_specs=[any_] * 7,
        out_specs=(vm,) * 4,
        scratch_shapes=[
            pltpu.SemaphoreType.REGULAR,
            pltpu.VMEM((CHUNKS, K, WIDTH), BF16),
            pltpu.VMEM((2, 3, 2, 1024), BF16),
            pltpu.VMEM((2, 3, 2, 1024), BF16),
            pltpu.VMEM((2, 3, 2, 1024), jnp.int32),
            pltpu.SMEM((2, 128), jnp.int32),
            pltpu.VMEM((CHUNKS, 8, WIDTH), F32),
            pltpu.VMEM((CHUNKS, 16, WIDTH), BF16),
            pltpu.VMEM((WIN * NEAR, WIDTH), BF16),
            pltpu.VMEM((LATE, WIDTH), BF16),
            pltpu.VMEM((WIN * NEAR, 256), F32),
            pltpu.VMEM((LATE, K), F32),
            pltpu.VMEM((6, NEAR, 128), BF16),
            pltpu.VMEM((2, 2, NEAR, 128), BF16),
            pltpu.VMEM((6, 64, 256), BF16),
            pltpu.VMEM((2, 2, 64, 256), BF16),
            pltpu.VMEM((6, 1, 256), F32),
            pltpu.VMEM((2, 2, 1, 256), F32),
            pltpu.VMEM((4, 2, NEAR, 128), BF16),
            pltpu.VMEM((4, 2, 64, 256), BF16),
            pltpu.VMEM((4, 2, 1, 256), F32),
            pltpu.VMEM((2, K, K), F32),
            pltpu.VMEM((2, K, 8, 128), BF16),
            pltpu.VMEM((2, K, K), F32),
            pltpu.VMEM((128, 128), F32),
            dma((5,)),
            dma,
            dma((3,)),
            dma((3,)),
            dma((2, 4, 3)),
            dma((2, 4, 3)),
            *[dma((2,))] * 6,
            *[dma((3,))] * 6,
        ],
        compiler_params=pltpu.CompilerParams(
            collective_id=0, has_side_effects=True, vmem_limit_bytes=32 * 1024 * 1024
        ),
        name="gather",
    )(obs_anom, obs_prec, innov, obs_column, cutoff, state_anom, root_far)
    return pl.pallas_call(
        analysis_kernel,
        out_shape=jax.ShapeDtypeStruct(state_anom.shape, BF16),
        in_specs=[vm] * 6,
        out_specs=any_,
        scratch_shapes=[pltpu.VMEM((2, K * 8, 128), F32), pltpu.VMEM((2, K, 8, 128), BF16), dma((2,))],
        compiler_params=pltpu.CompilerParams(vmem_limit_bytes=32 * 1024 * 1024),
        name="analysis",
    )(gram, proj, square, inv_root, flat, state_mean)


def solution(mesh):
    in_specs = (
        P("tm", None, "space", "member", None),
        P("tm", None, "space", None),
        P("tm", None, "space", None),
        P("tm", None, "space", None),
        P(),
        P("tm", "space", None, None),
        P("tm", "space", None, "member", None),
        P("tm", "space", "member", None),
    )
    out_specs = P("tm", "space", None, "member", None)
    return jax.shard_map(body, mesh=mesh, in_specs=in_specs, out_specs=out_specs, check_vma=False)
```
